32 devices in a mesh: pat: 2 (over y), slab: 4 (over z), phase: 2 (over x), enc: 2 (over core).
Axes of the slice: x: 2, y: 2, z: 4, core: 2. Of those that a mesh axis runs over, the one named last changes fastest.
Arguments:
- kspace_data: bfloat16 [4, 2, 4, 96, 64, 192], P('pat', 'phase', 'enc', 'slab'), parts along dimension 0, may hold values from -6 to 6
- coil_maps: bfloat16 [4, 24, 4, 64, 192], P('pat', None, None, 'slab'), parts along dimension 0, may hold values from -1 to 1
- sampling: int32 [2, 4, 128, 192], P('phase', 'enc', 'pat'), parts along dimension 2, may hold values 0 or 1
Outputs:
- image_estimate: float32 [4, 2, 4, 4, 64, 192], P('pat', 'phase', 'enc', None, 'slab'), parts along dimension 0
- residual: float32 [4, 2, 4, 96, 64, 192], P('pat', 'phase', 'enc', 'slab'), parts along dimension 0
The draws below stay inside these ranges and needn't reach their ends.
There are 2 independent parts, one for each index of `pat`. The reference program is written for one: setup_inputs(seed, part) draws one part's arguments, and reference() takes and returns one part's arrays. A program takes and returns all parts, laid end to end along the dimension named above; each array names one. Nothing has to cross between parts.
All inputs are finite; a program needn't handle non-finite values. No bound on the sum of `sampling` on one device may be relied on, other than what follows from the above.
Results may differ from the reference program's by a relative error of at most 0.0046.
Values may be sent and summed in bfloat16 or wider, within the bound.
A program may use at most 64 MiB of HBM per device.

```python
import math
import jax
import jax.numpy as jnp
from jax import lax

NY = 192
NZ = 64
COILS = 24
ENC = 4
NXW = 4
ITERS = 2
PHASES = 2
ROWS = 96


def draw_coil_maps(key, part):
    shape = (2, COILS, NXW, NZ, NY)
    coil_level = 1.0 + 2.0 * jnp.arange(COILS, dtype=jnp.float32) / max(COILS - 1, 1)
    depth_level = 1.0 + 2.0 * jnp.arange(NZ, dtype=jnp.float32) / max(NZ - 1, 1)
    envelope = jnp.sqrt(coil_level[:, None, None, None] * depth_level[None, None, :, None])
    entries = jax.random.normal(key, shape, jnp.float32)
    values = entries * envelope[None] / jnp.sqrt(8.0 * COILS)
    return jnp.clip(values, -1.0, 1.0).astype(jnp.bfloat16)


def plant(values, own_key, low, largest):
    longest = values.shape.index(max(values.shape))
    spots = []
    for shift in (0, 1):
        where = [jax.random.randint(jax.random.fold_in(own_key, axis), (), 0, length) for axis, length in enumerate(values.shape)]
        where[longest] = (where[longest] + shift) % values.shape[longest]
        spots.append(tuple(where))
    return values.at[spots[0]].set(low).at[spots[1]].set(largest)


def level_of(rng, dims, cuts, least, top_value):
    def one(dim, shards_of):
        steps = jax.random.uniform(jax.random.fold_in(jax.random.fold_in(rng, 6), dim), (shards_of,), jnp.float32, least / len(cuts), top_value / len(cuts))
        return jnp.repeat(jnp.exp(steps), dims[dim] // shards_of).reshape((-1,) + (1,) * (len(dims) - dim - 1))

    factor_of = one(*cuts[0])
    for cut in cuts[1:]:
        factor_of = factor_of * one(*cut)
    return factor_of


def centred(stream_key, dims, scale, most, shards=(), held_as=jnp.bfloat16):
    loudness = level_of(stream_key, dims, shards, -0.22, 0.18) if shards else 1.0
    drawn = jax.random.normal(stream_key, dims, jnp.float32) * scale * loudness
    return jnp.minimum(jnp.maximum(drawn, -most), most).astype(held_as)


def setup_inputs(seed: int = 0, part: int = 0) -> dict:
    key_list = jax.random.split(jax.random.key(seed), 4)
    part_splits = jax.random.split(jax.random.fold_in(key_list[3], part), 4)
    kspace_data = centred(part_splits[0], (2, PHASES, ENC, ROWS, NZ, NY), 1.0, 6.0, ((1, 2), (2, 2), (3, 4)))
    coil_maps = draw_coil_maps(jax.random.fold_in(jax.random.fold_in(key_list[3], part), 71), part)
    sampling = plant((jax.random.randint(part_splits[2], (PHASES, ENC, NZ, NY), 0, 3) < 1).astype(jnp.int32), jax.random.fold_in(part_splits[2], 1), 0, 1)
    return dict(kspace_data=kspace_data, coil_maps=coil_maps, sampling=sampling)


tv_weight = 0.15
smoothing = 0.6

def dft_table(length, direction):
    counter = jnp.arange(length, dtype=jnp.int32)
    product = counter[:, None] * counter[None, :] % length
    angle = product.astype(jnp.float32) * (2.0 * math.pi / length)
    factor = 1.0 / math.sqrt(length)
    return ((jnp.cos(angle) * factor).astype(jnp.bfloat16), (direction * jnp.sin(angle) * factor).astype(jnp.bfloat16))

def rounded(values):
    return lax.optimization_barrier(values.astype(jnp.bfloat16))

def along_rows(real_part, imag_part, table):
    cosine = table[0].astype(jnp.float32)
    sine = table[1].astype(jnp.float32)
    first = real_part.astype(jnp.float32)
    second = imag_part.astype(jnp.float32)
    real_out = jnp.einsum('...y,yw->...w', first, cosine) - jnp.einsum('...y,yw->...w', second, sine)
    imag_out = jnp.einsum('...y,yw->...w', first, sine) + jnp.einsum('...y,yw->...w', second, cosine)
    return (real_out, imag_out)

def along_depth(real_part, imag_part, table):
    cosine = table[0].astype(jnp.float32)
    sine = table[1].astype(jnp.float32)
    first = real_part.astype(jnp.float32)
    second = imag_part.astype(jnp.float32)
    real_out = jnp.einsum('...zy,zw->...wy', first, cosine) - jnp.einsum('...zy,zw->...wy', second, sine)
    imag_out = jnp.einsum('...zy,zw->...wy', first, sine) + jnp.einsum('...zy,zw->...wy', second, cosine)
    return (real_out, imag_out)

def forward_phase(values, sampled_phase, coil_maps, tables):
    base = rounded(values).astype(jnp.float32)
    coil_real = coil_maps[0].astype(jnp.float32)
    coil_imag = coil_maps[1].astype(jnp.float32)
    real_in = base[0][:, None]
    imag_in = base[1][:, None]
    prod_real = rounded(coil_real * real_in - coil_imag * imag_in)
    prod_imag = rounded(coil_real * imag_in + coil_imag * real_in)
    mid_real, mid_imag = along_rows(prod_real, prod_imag, tables[0])
    mid_real = rounded(mid_real).reshape(ENC, ROWS, NZ, NY)
    mid_imag = rounded(mid_imag).reshape(ENC, ROWS, NZ, NY)
    out_real, out_imag = along_depth(mid_real, mid_imag, tables[1])
    weight = sampled_phase[:, None]
    return jnp.stack([out_real * weight, out_imag * weight])

def adjoint_phase(values, coil_maps, tables):
    low_real = rounded(values[0])
    low_imag = rounded(values[1])
    mid_real, mid_imag = along_depth(low_real, low_imag, tables[3])
    mid_real = rounded(mid_real).reshape(ENC, COILS, NXW, NZ, NY)
    mid_imag = rounded(mid_imag).reshape(ENC, COILS, NXW, NZ, NY)
    coil_real = coil_maps[0].astype(jnp.float32)
    coil_imag = coil_maps[1].astype(jnp.float32)
    fine_real, fine_imag = along_rows(mid_real, mid_imag, tables[2])
    grad_real = lax.optimization_barrier(jnp.sum(coil_real * fine_real + coil_imag * fine_imag, axis=1))
    grad_imag = lax.optimization_barrier(jnp.sum(coil_real * fine_imag - coil_imag * fine_real, axis=1))
    return jnp.stack([grad_real, grad_imag])

def total_variation(values):
    difference = jnp.roll(values, -1, axis=1) - values
    modulus = difference[0] * difference[0] + difference[1] * difference[1]
    weights = difference / jnp.sqrt(modulus + smoothing * smoothing)[None]
    return jnp.roll(weights, 1, axis=1) - weights

def reference(kspace_data, coil_maps, sampling):
    tables = (dft_table(NY, -1.0), dft_table(NZ, -1.0), dft_table(NY, 1.0), dft_table(NZ, 1.0))
    sampled = sampling.astype(jnp.float32)
    residual = -(kspace_data.astype(jnp.float32) * sampled[None, :, :, None])
    image_estimate = jnp.zeros((2, PHASES, ENC, NXW, NZ, NY), jnp.float32)
    for iteration in range(ITERS):
        moved = jnp.moveaxis(residual, 1, 0)
        adjoint = lax.map(lambda values: adjoint_phase(values, coil_maps, tables), moved)
        gradient = jnp.moveaxis(adjoint, 0, 1) + tv_weight * total_variation(image_estimate)
        grad_sq = jnp.sum(gradient * gradient)
        moved_grad = jnp.moveaxis(gradient, 1, 0)
        spectrum = lax.map(lambda pair: forward_phase(pair[0], pair[1], coil_maps, tables), (moved_grad, sampled))
        spectrum = jnp.moveaxis(spectrum, 0, 1)
        spec_sq = jnp.sum(spectrum * spectrum)
        alpha = grad_sq / (spec_sq + 4.0 * tv_weight / smoothing * grad_sq + 1e-06)
        image_estimate = image_estimate - alpha * gradient
        residual = residual - alpha * spectrum
    return (image_estimate, residual)
```

```python
import functools
import math

import jax
import jax.numpy as jnp
import numpy as np
from jax import lax
from jax.experimental import pallas as pl
from jax.experimental.pallas import tpu as pltpu
from jax.sharding import PartitionSpec as P

ITERS = 2


tv_weight = 0.15
smoothing = 0.6


def with_halo(value, sides, width):
    for axis, dim in sides:
        size, length = (lax.axis_size(axis), value.shape[dim])
        up = [(i, (i + 1) % size) for i in range(size)]
        down = [(j, i) for i, j in up]
        last = lax.slice_in_dim(value, length - width, length, axis=dim)
        first = lax.slice_in_dim(value, 0, width, axis=dim)
        before = lax.ppermute(last, axis, up)
        after = lax.ppermute(first, axis, down)
        value = jnp.concatenate([before, value, after], axis=dim)
    return value


def dft_table(length, direction):
    counter = jnp.arange(length, dtype=jnp.int32)
    product = counter[:, None] * counter[None, :] % length
    angle = product.astype(jnp.float32) * (2.0 * math.pi / length)
    factor = 1.0 / math.sqrt(length)
    return (
        (jnp.cos(angle) * factor).astype(jnp.bfloat16),
        (direction * jnp.sin(angle) * factor).astype(jnp.bfloat16),
    )


def along_rows(real_part, imag_part, table):
    cosine, sine = table
    real_out = jnp.matmul(real_part, cosine, preferred_element_type=jnp.float32) - jnp.matmul(
        imag_part, sine, preferred_element_type=jnp.float32
    )
    imag_out = jnp.matmul(real_part, sine, preferred_element_type=jnp.float32) + jnp.matmul(
        imag_part, cosine, preferred_element_type=jnp.float32
    )
    return (real_out, imag_out)


def along_depth(real_part, imag_part, table):
    cosine, sine = table
    real_out = jnp.einsum(
        "...zy,zw->...wy", real_part, cosine, preferred_element_type=jnp.float32
    ) - jnp.einsum("...zy,zw->...wy", imag_part, sine, preferred_element_type=jnp.float32)
    imag_out = jnp.einsum(
        "...zy,zw->...wy", real_part, sine, preferred_element_type=jnp.float32
    ) + jnp.einsum("...zy,zw->...wy", imag_part, cosine, preferred_element_type=jnp.float32)
    return (real_out, imag_out)


def coil_product(coil_real, coil_imag, real_in, imag_in, column_fwd):
    prod_real = (coil_real * real_in - coil_imag * imag_in).astype(jnp.bfloat16)
    prod_imag = (coil_real * imag_in + coil_imag * real_in).astype(jnp.bfloat16)
    mid_real, mid_imag = along_rows(prod_real, prod_imag, column_fwd)
    return jnp.stack([mid_real, mid_imag]).astype(jnp.bfloat16)


def body(kspace_data, coil_maps, sampling):
    phases = kspace_data.shape[1]
    encodings = kspace_data.shape[2]
    coils = coil_maps.shape[1]
    readout = coil_maps.shape[2]
    zdepth = coil_maps.shape[3]
    lines = coil_maps.shape[4]
    slices = kspace_data.shape[4]
    column_fwd = dft_table(lines, -1.0)
    depth_fwd = dft_table(slices, -1.0)
    column_inv = dft_table(lines, 1.0)
    depth_inv = dft_table(slices, 1.0)
    coil_real = coil_maps[0].astype(jnp.float32)
    coil_imag = coil_maps[1].astype(jnp.float32)
    sampled = sampling.astype(jnp.float32)[None, :, :, None]
    residual = -(kspace_data.astype(jnp.float32) * sampled)
    image_estimate = jnp.zeros((2, phases, encodings, readout, zdepth, lines), jnp.float32)
    row_count = kspace_data.shape[3]
    coil_rows = lax.all_to_all(
        coil_maps.reshape(2, coils * readout, zdepth, lines),
        "slab",
        split_axis=1,
        concat_axis=2,
        tiled=True,
    )
    row_columns = (
        lax.axis_index("slab") * row_count + jnp.arange(row_count, dtype=jnp.int32)
    ) % readout
    for iteration in range(ITERS):
        low = residual.astype(jnp.bfloat16)
        inv_real, inv_imag = along_depth(low[0], low[1], depth_inv)
        partial_rows = jnp.stack([inv_real, inv_imag]).astype(jnp.bfloat16)
        portion = lax.all_to_all(partial_rows, "slab", split_axis=4, concat_axis=3, tiled=True)
        shaped = portion.reshape(
            2,
            portion.shape[1],
            portion.shape[2],
            coils,
            readout,
            portion.shape[4],
            portion.shape[5],
        )
        fine_real, fine_imag = along_rows(shaped[0], shaped[1], column_inv)
        grad_real = jnp.sum(coil_real * fine_real + coil_imag * fine_imag, axis=2)
        grad_imag = jnp.sum(coil_real * fine_imag - coil_imag * fine_real, axis=2)
        adjoint = jnp.stack([grad_real, grad_imag])
        padded = with_halo(image_estimate, (("phase", 1),), 1)
        difference = padded[:, 1:] - padded[:, :-1]
        modulus = difference[0] * difference[0] + difference[1] * difference[1]
        weights = difference / jnp.sqrt(modulus + smoothing * smoothing)[None]
        gradient = adjoint + tv_weight * (weights[:, :-1] - weights[:, 1:])
        grad_local = jnp.sum(gradient * gradient)
        grad_sq = lax.psum(grad_local, ("slab", "phase", "enc"))
        low_grad = gradient.astype(jnp.bfloat16)
        picked = jnp.take(
            lax.all_gather(low_grad, "slab", axis=4, tiled=True), row_columns, axis=3
        ).astype(jnp.float32)
        local_coils = coil_rows.astype(jnp.float32)
        mid = coil_product(local_coils[0], local_coils[1], picked[0], picked[1], column_fwd)
        out_real, out_imag = along_depth(mid[0], mid[1], depth_fwd)
        spectrum = jnp.stack([out_real, out_imag])
        spectrum = spectrum * sampled
        spec_local = jnp.sum(spectrum * spectrum)
        spec_sq = lax.psum(spec_local, ("slab", "phase", "enc"))
        alpha = grad_sq / (spec_sq + 4.0 * tv_weight / smoothing * grad_sq + 1e-06)
        image_estimate = image_estimate - alpha * gradient
        residual = residual - alpha * spectrum
    return (image_estimate, residual)


MESH = pl.DeviceIdType.MESH
LAG = 3


def host_table(length):
    counter = np.arange(length)
    angle = (counter[:, None] * counter[None, :] % length).astype(np.float32) * np.float32(
        2.0 * math.pi / length
    )
    factor = np.float32(1.0 / math.sqrt(length))
    return (
        (np.cos(angle) * factor).astype(jnp.bfloat16),
        (np.sin(angle) * factor).astype(jnp.bfloat16),
    )


def fused(sizes, k_ref, coil_ref, samp_ref, cy_ref, sy_ref, ti_ref, tf_ref, img_ref, res_ref,
          rows_ref, mask_ref, q_ref, e_ref, rs_ref, rr_ref, own_ref, ag_ref, g_ref, tv_ref,
          ar_ref, gg_ref, ee_ref,
          own_sem, cz_send, cz_recv, cx_send, cx_recv, cc_send, cc_recv,
          rs_send, rs_recv, ag_send, ag_recv, tv_send, tv_recv, ar_send, ar_recv):
    n, nphase, nenc = sizes
    readout, depth = coil_ref.shape[2], coil_ref.shape[3]
    encs = k_ref.shape[2]
    slices, lines = k_ref.shape[4], k_ref.shape[5]
    coils = k_ref.shape[3] // readout
    pieces = encs * readout
    me = lax.axis_index("slab")
    ph = lax.axis_index("phase")
    en = lax.axis_index("enc")
    f32, bf16 = jnp.float32, jnp.bfloat16

    def wrap(value, size):
        return lax.rem(value + size, size)

    offsets = [
        (a, b, c)
        for a in range(n)
        for b in range(nphase)
        for c in range(nenc)
        if (a, b, c) != (0, 0, 0)
    ]

    def rel(a, b, c):
        return {"slab": wrap(me + a, n), "phase": wrap(ph + b, nphase), "enc": wrap(en + c, nenc)}

    def remote(src, dst, send, recv, where):
        return pltpu.make_async_remote_copy(
            src_ref=src, dst_ref=dst, send_sem=send, recv_sem=recv, device_id=where,
            device_id_type=MESH,
        )

    barrier = pltpu.get_barrier_semaphore()
    for off in offsets:
        pl.semaphore_signal(barrier, inc=1, device_id=rel(*off), device_id_type=MESH)
    pl.semaphore_wait(barrier, len(offsets))

    quarter = ph * nenc + en
    across = wrap(ph + 1, nphase) * nenc + en

    def coil_z(k):
        to = wrap(me + k, n)
        return remote(
            coil_ref.at[:, pl.ds(to * coils, coils), quarter], rows_ref.at[me, :, :, quarter],
            cz_send.at[k - 1], cz_recv.at[k - 1], rel(k, 0, 0),
        )

    def coil_z_in(k):
        frm = wrap(me - k, n)
        return remote(
            coil_ref.at[:, pl.ds(0, coils), quarter], rows_ref.at[frm, :, :, quarter],
            cz_send.at[k - 1], cz_recv.at[k - 1], rel(k, 0, 0),
        )

    def coil_x(k, which):
        at = rows_ref.at[wrap(me - k, n), :, :, which]
        return remote(at, at, cx_send.at[k - 1], cx_recv.at[k - 1], rel(0, 1, 0))

    def coil_c(k, which, s):
        at = rows_ref.at[wrap(me - k, n), :, :, which]
        return remote(at, at, cc_send.at[s, k - 1], cc_recv.at[s, k - 1], rel(0, 0, 1))

    for k in range(1, n):
        coil_z(k).start()
    mine = pltpu.make_async_copy(
        coil_ref.at[:, pl.ds(me * coils, coils)], rows_ref.at[me], own_sem
    )
    mine.start()

    mask_ref[...] = samp_ref[0].astype(f32)
    gg_ref[...] = jnp.zeros_like(gg_ref)
    ee_ref[...] = jnp.zeros_like(ee_ref)

    def transform(i, alpha):
        e, x = i // readout, lax.rem(i, readout)
        mask = mask_ref[e]
        mids = []
        for c in range(coils):
            r = c * readout + x
            parts = []
            for ri in range(2):
                value = -(k_ref[ri, 0, e, r].astype(f32) * mask)
                if alpha is not None:
                    value = value - alpha * e_ref[i, c, ri]
                    res_ref[ri, 0, e, r] = value
                parts.append(value.astype(bf16))
            stacked = jnp.concatenate(parts, axis=0)
            mids.append(
                jnp.dot(ti_ref[...], stacked, preferred_element_type=f32).astype(bf16)
            )
        mid = jnp.concatenate(mids, axis=0)
        a = jnp.dot(mid, cy_ref[...], preferred_element_type=f32)
        b = jnp.dot(mid, sy_ref[...], preferred_element_type=f32)
        for c in range(coils):
            lo = 2 * slices * c
            hi = lo + slices
            q_ref[i, c, 0] = a[lo : lo + slices] - b[hi : hi + slices]
            q_ref[i, c, 1] = b[lo : lo + slices] + a[hi : hi + slices]

    def coil_of(c, x):
        return [
            jnp.concatenate([rows_ref[b, ri, c, x] for b in range(n)], axis=0).astype(f32)
            for ri in range(2)
        ]

    def rs_copy(it, i, k):
        return remote(
            rs_ref.at[it, i, wrap(me + k, n)], rr_ref.at[it, i, k - 1],
            rs_send.at[i, k - 1], rs_recv.at[i, k - 1], rel(k, 0, 0),
        )

    def ag_copy(it, i, k):
        return remote(
            ag_ref.at[it, i, me], ag_ref.at[it, i, me],
            ag_send.at[i, k - 1], ag_recv.at[i, k - 1], rel(k, 0, 0),
        )

    def ag_in(it, i, k):
        at = ag_ref.at[it, i, wrap(me - k, n)]
        return remote(at, at, ag_send.at[i, k - 1], ag_recv.at[i, k - 1], rel(k, 0, 0))

    def tv_copy(i):
        return remote(g_ref.at[0, i], tv_ref.at[i], tv_send.at[i], tv_recv.at[i], rel(0, 1, 0))

    def combine(it, i):
        x = lax.rem(i, readout)
        pr = jnp.zeros((slices, lines), f32)
        pi = jnp.zeros((slices, lines), f32)
        for c in range(coils):
            cr, ci = coil_of(c, x)
            qr, qi = q_ref[i, c, 0], q_ref[i, c, 1]
            pr += cr * qr + ci * qi
            pi += cr * qi - ci * qr
        for b in range(n):
            for ri, part in enumerate((pr, pi)):
                cut = part[b * depth : (b + 1) * depth]
                own_ref[i, b, ri] = cut
                rs_ref[it, i, b, ri] = cut.astype(bf16)
        for k in range(1, n):
            rs_copy(it, i, k).start()

    def reduce(it, i, alpha):
        for k in range(1, n):
            rs_copy(it, i, k).wait_recv()
        grads = []
        for ri in range(2):
            total = own_ref[i, me, ri]
            for k in range(1, n):
                total = total + rr_ref[it, i, k - 1, ri].astype(f32)
            grads.append(total)
        if it > 0:
            tv_copy(i).wait_recv()
            dr = -alpha * (tv_ref[i, 0] - g_ref[0, i, 0])
            di = -alpha * (tv_ref[i, 1] - g_ref[0, i, 1])
            scale = (-2.0 * tv_weight) / jnp.sqrt(dr * dr + di * di + smoothing * smoothing)
            grads = [grads[0] + dr * scale, grads[1] + di * scale]
        for ri in range(2):
            g_ref[it, i, ri] = grads[ri]
            ag_ref[it, i, me, ri] = grads[ri].astype(bf16)
        gg_ref[...] += grads[0] * grads[0] + grads[1] * grads[1]
        for k in range(1, n):
            ag_copy(it, i, k).start()
        if it == 0:
            tv_copy(i).start()

    def forward(it, i):
        e, x = i // readout, lax.rem(i, readout)
        for k in range(1, n):
            ag_in(it, i, k).wait_recv()
        vr, vi = [
            jnp.concatenate([ag_ref[it, i, b, ri] for b in range(n)], axis=0).astype(f32)
            for ri in range(2)
        ]
        prods = []
        for c in range(coils):
            cr, ci = coil_of(c, x)
            prods.append((cr * vr - ci * vi).astype(bf16))
            prods.append((cr * vi + ci * vr).astype(bf16))
        prod = jnp.concatenate(prods, axis=0)
        a = jnp.dot(prod, cy_ref[...], preferred_element_type=f32)
        b = jnp.dot(prod, sy_ref[...], preferred_element_type=f32)
        mask = mask_ref[e]
        total = jnp.zeros((slices, lines), f32)
        for c in range(coils):
            lo = 2 * slices * c
            hi = lo + slices
            mid = jnp.concatenate(
                [
                    (a[lo : lo + slices] + b[hi : hi + slices]).astype(bf16),
                    (a[hi : hi + slices] - b[lo : lo + slices]).astype(bf16),
                ],
                axis=0,
            )
            out = jnp.dot(tf_ref[...], mid, preferred_element_type=f32)
            er, ei = out[:slices] * mask, out[slices:] * mask
            e_ref[i, c, 0] = er
            e_ref[i, c, 1] = ei
            total += er * er + ei * ei
        ee_ref[...] += total

    flat = (me * nphase + ph) * nenc + en

    def ar_copy(it, j):
        return remote(
            ar_ref.at[it, flat], ar_ref.at[it, flat], ar_send.at[it, j], ar_recv.at[it, j],
            rel(*offsets[j]),
        )

    def ar_in(it, j):
        a, b, c = offsets[j]
        frm = (wrap(me - a, n) * nphase + wrap(ph - b, nphase)) * nenc + wrap(en - c, nenc)
        at = ar_ref.at[it, frm]
        return remote(at, at, ar_send.at[it, j], ar_recv.at[it, j], rel(*offsets[j]))

    def step_size(it):
        gg = jnp.sum(jnp.sum(gg_ref[...], axis=0, keepdims=True), axis=1, keepdims=True)
        ee = jnp.sum(jnp.sum(ee_ref[...], axis=0, keepdims=True), axis=1, keepdims=True)
        row = lax.broadcasted_iota(jnp.int32, ar_ref.shape[2:], 0)
        ar_ref[it, flat] = jnp.where(row == 0, gg, ee)
        for j in range(len(offsets)):
            ar_copy(it, j).start()
        gg_ref[...] = jnp.zeros_like(gg_ref)
        ee_ref[...] = jnp.zeros_like(ee_ref)
        for j in range(len(offsets)):
            ar_in(it, j).wait_recv()
        total = ar_ref[it, 0]
        for s in range(1, n * nphase * nenc):
            total = total + ar_ref[it, s]
        gg, ee = total[0:1, 0:1], total[1:2, 0:1]
        return gg / (ee + 4.0 * tv_weight / smoothing * gg + 1e-06)

    def finish_sends(it):
        @pl.loop(0, pieces)
        def _(i):
            for k in range(1, n):
                rs_copy(it, i, k).wait_send()
                ag_copy(it, i, k).wait_send()
            if it == 0:
                tv_copy(i).wait_send()

        for j in range(len(offsets)):
            ar_copy(it, j).wait_send()

    def sweep(it, alpha):
        @pl.loop(0, pieces + 2 * LAG)
        def _(s):
            @pl.when(s < pieces)
            def _():
                if it > 0:
                    transform(s, alpha)
                combine(it, s)

            @pl.when((s >= LAG) & (s < pieces + LAG))
            def _():
                reduce(it, s - LAG, alpha)

            @pl.when(s >= 2 * LAG)
            def _():
                forward(it, s - 2 * LAG)

    @pl.loop(0, pieces)
    def _(i):
        transform(i, None)

    for k in range(1, n):
        coil_z_in(k).wait_recv()
        coil_x(k, quarter).start()
        coil_c(k, quarter, 0).start()
    for k in range(1, n):
        coil_x(k, across).wait_recv()
        coil_c(k, across, 1).start()
    mine.wait()
    partner = wrap(en + 1, nenc)
    for k in range(1, n):
        coil_c(k, ph * nenc + partner, 0).wait_recv()
        coil_c(k, wrap(ph + 1, nphase) * nenc + partner, 1).wait_recv()

    sweep(0, None)
    alpha0 = step_size(0)
    finish_sends(0)
    sweep(1, alpha0)
    alpha1 = step_size(1)

    for ri in range(2):
        for i in range(pieces):
            img_ref[ri, 0, i // readout, i % readout] = (
                -alpha0 * g_ref[0, i, ri] - alpha1 * g_ref[1, i, ri]
            )

    @pl.loop(0, pieces)
    def _(i):
        e, x = i // readout, lax.rem(i, readout)
        for c in range(coils):
            r = c * readout + x
            for ri in range(2):
                res_ref[ri, 0, e, r] = res_ref[ri, 0, e, r] - alpha1 * e_ref[i, c, ri]

    finish_sends(1)
    for k in range(1, n):
        coil_z(k).wait_send()
        coil_x(k, quarter).wait_send()
        coil_c(k, quarter, 0).wait_send()
        coil_c(k, across, 1).wait_send()


def fused_body(shape, kspace_data, coil_maps, sampling):
    n, nphase, nenc = shape["slab"], shape["phase"], shape["enc"]
    encs, row_count, slices, lines = kspace_data.shape[2:]
    readout, depth = coil_maps.shape[2:4]
    coils = row_count // readout
    pieces = encs * readout
    group = n * nphase * nenc
    cy, sy = host_table(lines)
    cz, sz = host_table(slices)
    inv = np.block([[cz, -sz], [sz, cz]])
    fwd = np.block([[cz, sz], [-sz, cz]])
    f32, bf16 = jnp.float32, jnp.bfloat16
    dma = pltpu.SemaphoreType.DMA
    vmem = pl.BlockSpec(memory_space=pltpu.VMEM)
    return pl.pallas_call(
        functools.partial(fused, (n, nphase, nenc)),
        out_shape=[
            jax.ShapeDtypeStruct((2, 1, encs, readout, depth, lines), f32),
            jax.ShapeDtypeStruct(kspace_data.shape, f32),
        ],
        in_specs=[vmem] * 7,
        out_specs=[vmem] * 2,
        scratch_shapes=[
            pltpu.VMEM((n, 2, coils, readout, depth, lines), bf16),
            pltpu.VMEM((encs, slices, lines), f32),
            pltpu.VMEM((pieces, coils, 2, slices, lines), f32),
            pltpu.VMEM((pieces, coils, 2, slices, lines), f32),
            pltpu.VMEM((ITERS, pieces, n, 2, depth, lines), bf16),
            pltpu.VMEM((ITERS, pieces, n - 1, 2, depth, lines), bf16),
            pltpu.VMEM((pieces, n, 2, depth, lines), f32),
            pltpu.VMEM((ITERS, pieces, n, 2, depth, lines), bf16),
            pltpu.VMEM((ITERS, pieces, 2, depth, lines), f32),
            pltpu.VMEM((pieces, 2, depth, lines), f32),
            pltpu.VMEM((ITERS, group, 8, 128), f32),
            pltpu.VMEM((depth, lines), f32),
            pltpu.VMEM((slices, lines), f32),
            dma,
            dma((n - 1,)),
            dma((n - 1,)),
            dma((n - 1,)),
            dma((n - 1,)),
            dma((2, n - 1)),
            dma((2, n - 1)),
            dma((pieces, n - 1)),
            dma((pieces, n - 1)),
            dma((pieces, n - 1)),
            dma((pieces, n - 1)),
            dma((pieces,)),
            dma((pieces,)),
            dma((ITERS, group - 1)),
            dma((ITERS, group - 1)),
        ],
        compiler_params=pltpu.CompilerParams(
            collective_id=0, has_side_effects=True, vmem_limit_bytes=60 * 1024 * 1024
        ),
    )(kspace_data, coil_maps, sampling, jnp.asarray(cy), jnp.asarray(sy), jnp.asarray(inv), jnp.asarray(fwd))


def chosen(shape, kspace_data, coil_maps, sampling):
    readout, depth = coil_maps.shape[2:4]
    fits = (
        shape["phase"] == 2
        and kspace_data.shape[1] == 1
        and shape["enc"] == 2
        and readout == shape["phase"] * shape["enc"]
        and kspace_data.shape[3] % readout == 0
        and depth % 16 == 0
        and shape["slab"] > 1
    )
    if fits:
        return fused_body(shape, kspace_data, coil_maps, sampling)
    return body(kspace_data, coil_maps, sampling)


def solution(mesh):
    in_specs = (
        P("pat", "phase", "enc", "slab", None, None),
        P("pat", None, None, "slab", None),
        P("phase", "enc", "pat", None),
    )
    out_specs = (
        P("pat", "phase", "enc", None, "slab", None),
        P("pat", "phase", "enc", "slab", None, None),
    )
    return jax.shard_map(functools.partial(chosen, dict(mesh.shape)), mesh=mesh, in_specs=in_specs, out_specs=out_specs, check_vma=False)
```

```python
import functools
import math

import jax
import jax.numpy as jnp
import numpy as np
from jax import lax
from jax.experimental import pallas as pl
from jax.experimental.pallas import tpu as pltpu
from jax.sharding import PartitionSpec as P

ITERS = 2


tv_weight = 0.15
smoothing = 0.6


def with_halo(value, sides, width):
    for axis, dim in sides:
        size, length = (lax.axis_size(axis), value.shape[dim])
        up = [(i, (i + 1) % size) for i in range(size)]
        down = [(j, i) for i, j in up]
        last = lax.slice_in_dim(value, length - width, length, axis=dim)
        first = lax.slice_in_dim(value, 0, width, axis=dim)
        before = lax.ppermute(last, axis, up)
        after = lax.ppermute(first, axis, down)
        value = jnp.concatenate([before, value, after], axis=dim)
    return value


def dft_table(length, direction):
    counter = jnp.arange(length, dtype=jnp.int32)
    product = counter[:, None] * counter[None, :] % length
    angle = product.astype(jnp.float32) * (2.0 * math.pi / length)
    factor = 1.0 / math.sqrt(length)
    return (
        (jnp.cos(angle) * factor).astype(jnp.bfloat16),
        (direction * jnp.sin(angle) * factor).astype(jnp.bfloat16),
    )


def along_rows(real_part, imag_part, table):
    cosine, sine = table
    real_out = jnp.matmul(real_part, cosine, preferred_element_type=jnp.float32) - jnp.matmul(
        imag_part, sine, preferred_element_type=jnp.float32
    )
    imag_out = jnp.matmul(real_part, sine, preferred_element_type=jnp.float32) + jnp.matmul(
        imag_part, cosine, preferred_element_type=jnp.float32
    )
    return (real_out, imag_out)


def along_depth(real_part, imag_part, table):
    cosine, sine = table
    real_out = jnp.einsum(
        "...zy,zw->...wy", real_part, cosine, preferred_element_type=jnp.float32
    ) - jnp.einsum("...zy,zw->...wy", imag_part, sine, preferred_element_type=jnp.float32)
    imag_out = jnp.einsum(
        "...zy,zw->...wy", real_part, sine, preferred_element_type=jnp.float32
    ) + jnp.einsum("...zy,zw->...wy", imag_part, cosine, preferred_element_type=jnp.float32)
    return (real_out, imag_out)


def coil_product(coil_real, coil_imag, real_in, imag_in, column_fwd):
    prod_real = (coil_real * real_in - coil_imag * imag_in).astype(jnp.bfloat16)
    prod_imag = (coil_real * imag_in + coil_imag * real_in).astype(jnp.bfloat16)
    mid_real, mid_imag = along_rows(prod_real, prod_imag, column_fwd)
    return jnp.stack([mid_real, mid_imag]).astype(jnp.bfloat16)


def body(kspace_data, coil_maps, sampling):
    phases = kspace_data.shape[1]
    encodings = kspace_data.shape[2]
    coils = coil_maps.shape[1]
    readout = coil_maps.shape[2]
    zdepth = coil_maps.shape[3]
    lines = coil_maps.shape[4]
    slices = kspace_data.shape[4]
    column_fwd = dft_table(lines, -1.0)
    depth_fwd = dft_table(slices, -1.0)
    column_inv = dft_table(lines, 1.0)
    depth_inv = dft_table(slices, 1.0)
    coil_real = coil_maps[0].astype(jnp.float32)
    coil_imag = coil_maps[1].astype(jnp.float32)
    sampled = sampling.astype(jnp.float32)[None, :, :, None]
    residual = -(kspace_data.astype(jnp.float32) * sampled)
    image_estimate = jnp.zeros((2, phases, encodings, readout, zdepth, lines), jnp.float32)
    row_count = kspace_data.shape[3]
    coil_rows = lax.all_to_all(
        coil_maps.reshape(2, coils * readout, zdepth, lines),
        "slab",
        split_axis=1,
        concat_axis=2,
        tiled=True,
    )
    row_columns = (
        lax.axis_index("slab") * row_count + jnp.arange(row_count, dtype=jnp.int32)
    ) % readout
    for iteration in range(ITERS):
        low = residual.astype(jnp.bfloat16)
        inv_real, inv_imag = along_depth(low[0], low[1], depth_inv)
        partial_rows = jnp.stack([inv_real, inv_imag]).astype(jnp.bfloat16)
        portion = lax.all_to_all(partial_rows, "slab", split_axis=4, concat_axis=3, tiled=True)
        shaped = portion.reshape(
            2,
            portion.shape[1],
            portion.shape[2],
            coils,
            readout,
            portion.shape[4],
            portion.shape[5],
        )
        fine_real, fine_imag = along_rows(shaped[0], shaped[1], column_inv)
        grad_real = jnp.sum(coil_real * fine_real + coil_imag * fine_imag, axis=2)
        grad_imag = jnp.sum(coil_real * fine_imag - coil_imag * fine_real, axis=2)
        adjoint = jnp.stack([grad_real, grad_imag])
        padded = with_halo(image_estimate, (("phase", 1),), 1)
        difference = padded[:, 1:] - padded[:, :-1]
        modulus = difference[0] * difference[0] + difference[1] * difference[1]
        weights = difference / jnp.sqrt(modulus + smoothing * smoothing)[None]
        gradient = adjoint + tv_weight * (weights[:, :-1] - weights[:, 1:])
        grad_local = jnp.sum(gradient * gradient)
        grad_sq = lax.psum(grad_local, ("slab", "phase", "enc"))
        low_grad = gradient.astype(jnp.bfloat16)
        picked = jnp.take(
            lax.all_gather(low_grad, "slab", axis=4, tiled=True), row_columns, axis=3
        ).astype(jnp.float32)
        local_coils = coil_rows.astype(jnp.float32)
        mid = coil_product(local_coils[0], local_coils[1], picked[0], picked[1], column_fwd)
        out_real, out_imag = along_depth(mid[0], mid[1], depth_fwd)
        spectrum = jnp.stack([out_real, out_imag])
        spectrum = spectrum * sampled
        spec_local = jnp.sum(spectrum * spectrum)
        spec_sq = lax.psum(spec_local, ("slab", "phase", "enc"))
        alpha = grad_sq / (spec_sq + 4.0 * tv_weight / smoothing * grad_sq + 1e-06)
        image_estimate = image_estimate - alpha * gradient
        residual = residual - alpha * spectrum
    return (image_estimate, residual)


MESH = pl.DeviceIdType.MESH
LAG = 3
HALF = 64
KEEP = pltpu.VMEM
LIMIT = 40 * 1024 * 1024
TAIL_LIMIT = 40 * 1024 * 1024


def host_table(length):
    counter = np.arange(length)
    angle = (counter[:, None] * counter[None, :] % length).astype(np.float32) * np.float32(
        2.0 * math.pi / length
    )
    factor = np.float32(1.0 / math.sqrt(length))
    return (
        (np.cos(angle) * factor).astype(jnp.bfloat16),
        (np.sin(angle) * factor).astype(jnp.bfloat16),
    )


def packed(real, imag):
    full = real.shape[1] - HALF
    mixed = jnp.concatenate([real[:, full:], imag[:, full:]], axis=1)
    return [real[:, :full], imag[:, :full], mixed]


def unpacked(first, second, mixed):
    return (
        jnp.concatenate([first, mixed[:, :HALF]], axis=1),
        jnp.concatenate([second, mixed[:, HALF:]], axis=1),
    )


def finish(r_ref, e_ref, g_ref, a_ref, img_ref, res_ref, stage_ref, sems):
    readout = img_ref.shape[3]
    pieces, coils = e_ref.shape[:2]
    encs = img_ref.shape[2]
    alpha0, alpha1 = a_ref[0, 0:1, 0:1], a_ref[1, 0:1, 0:1]

    def out(ri, e):
        return pltpu.make_async_copy(stage_ref.at[ri, 0, e], res_ref.at[ri, 0, e], sems.at[ri, e])

    for ri in range(2):
        for e in range(encs):
            @pl.loop(0, readout)
            def _(x):
                for c in range(coils):
                    r = c * readout + x
                    stage_ref[ri, 0, e, r] = (
                        r_ref[ri, 0, e, r] - alpha1 * e_ref[e * readout + x, c, ri]
                    )

            out(ri, e).start()
    for i in range(pieces):
        parts = [-alpha0 * g_ref[0, i, t] - alpha1 * g_ref[1, i, t] for t in range(3)]
        real, imag = unpacked(*parts)
        img_ref[0, 0, i // readout, i % readout] = real
        img_ref[1, 0, i // readout, i % readout] = imag
    for ri in range(2):
        for e in range(encs):
            out(ri, e).wait()


def fused(sizes, k_hbm, coil_hbm, samp_hbm, cy_ref, sy_ref, ti_ref, tf_ref, res_ref, e_ref, g_ref,
          a_ref, k_ref, coil_ref, samp_ref, pack_ref,
          rows_ref, mask_ref, q_ref, rs_ref, rr_ref, own_ref, ag_ref, tv_ref,
          ar_ref, gg_ref, ee_ref,
          in_sem, cz_send, cz_recv, cx_send, cx_recv, cc_send, cc_recv,
          rs_send, rs_recv, ag_send, ag_recv, tv_send, tv_recv, ar_send, ar_recv):
    n, nphase, nenc = sizes
    readout, depth = coil_ref.shape[2], coil_ref.shape[3]
    encs = k_ref.shape[2]
    slices, lines = k_ref.shape[4], k_ref.shape[5]
    coils = k_ref.shape[3] // readout
    pieces = encs * readout
    me = lax.axis_index("slab")
    ph = lax.axis_index("phase")
    en = lax.axis_index("enc")
    f32, bf16 = jnp.float32, jnp.bfloat16

    def wrap(value, size):
        return lax.rem(value + size, size)

    offsets = [
        (a, b, c)
        for a in range(n)
        for b in range(nphase)
        for c in range(nenc)
        if (a, b, c) != (0, 0, 0)
    ]

    def rel(a, b, c):
        return {"slab": wrap(me + a, n), "phase": wrap(ph + b, nphase), "enc": wrap(en + c, nenc)}

    def remote(src, dst, send, recv, where):
        return pltpu.make_async_remote_copy(
            src_ref=src, dst_ref=dst, send_sem=send, recv_sem=recv, device_id=where,
            device_id_type=MESH,
        )

    barrier = pltpu.get_barrier_semaphore()
    for off in offsets:
        pl.semaphore_signal(barrier, inc=1, device_id=rel(*off), device_id_type=MESH)

    quarter = ph * nenc + en
    across = wrap(ph + 1, nphase) * nenc + en

    def coil_z(k):
        to = wrap(me + k, n)
        return remote(
            pack_ref.at[pl.ds(to * coils, coils)], rows_ref.at[me, :, quarter],
            cz_send.at[k - 1], cz_recv.at[k - 1], rel(k, 0, 0),
        )

    def coil_z_in(k):
        frm = wrap(me - k, n)
        return remote(
            pack_ref.at[pl.ds(0, coils)], rows_ref.at[frm, :, quarter],
            cz_send.at[k - 1], cz_recv.at[k - 1], rel(k, 0, 0),
        )

    def coil_x(k, which):
        at = rows_ref.at[wrap(me - k, n), :, which]
        return remote(at, at, cx_send.at[k - 1], cx_recv.at[k - 1], rel(0, 1, 0))

    def coil_c(k, which, s):
        at = rows_ref.at[wrap(me - k, n), :, which]
        return remote(at, at, cc_send.at[s, k - 1], cc_recv.at[s, k - 1], rel(0, 0, 1))

    def load_k(e):
        return pltpu.make_async_copy(k_hbm.at[:, :, e], k_ref.at[:, :, e], in_sem.at[2 + e])

    load_coil = pltpu.make_async_copy(coil_hbm, coil_ref, in_sem.at[0])
    load_samp = pltpu.make_async_copy(samp_hbm, samp_ref, in_sem.at[1])
    load_coil.start()
    load_samp.start()
    for e in range(encs):
        load_k(e).start()
    load_coil.wait()

    @pl.loop(0, coils * n)
    def _(c):
        for t, part in enumerate(packed(coil_ref[0, c, quarter].astype(f32), coil_ref[1, c, quarter].astype(f32))):
            pack_ref[c, t] = part.astype(bf16)

    @pl.loop(0, coils)
    def _(c):
        source = me * coils + c
        for x in range(readout):
            parts = packed(coil_ref[0, source, x].astype(f32), coil_ref[1, source, x].astype(f32))
            for t, part in enumerate(parts):
                rows_ref[me, c, x, t] = part.astype(bf16)

    load_samp.wait()
    mask_ref[...] = samp_ref[0].astype(f32)
    gg_ref[...] = jnp.zeros_like(gg_ref)
    ee_ref[...] = jnp.zeros_like(ee_ref)

    def transform(i, alpha):
        e, x = i // readout, lax.rem(i, readout)
        mask = mask_ref[e]
        mids = []
        for c in range(coils):
            r = c * readout + x
            parts = []
            for ri in range(2):
                value = -(k_ref[ri, 0, e, r].astype(f32) * mask)
                if alpha is not None:
                    value = value - alpha * e_ref[i, c, ri]
                    res_ref[ri, 0, e, r] = value
                parts.append(value.astype(bf16))
            stacked = jnp.concatenate(parts, axis=0)
            mids.append(
                jnp.dot(ti_ref[...], stacked, preferred_element_type=f32).astype(bf16)
            )
        mid = jnp.concatenate(mids, axis=0)
        a = jnp.dot(mid, cy_ref[...], preferred_element_type=f32)
        b = jnp.dot(mid, sy_ref[...], preferred_element_type=f32)
        for c in range(coils):
            lo = 2 * slices * c
            hi = lo + slices
            q_ref[i, c, 0] = a[lo : lo + slices] - b[hi : hi + slices]
            q_ref[i, c, 1] = b[lo : lo + slices] + a[hi : hi + slices]

    def coil_of(c, x):
        return unpacked(*[
            jnp.concatenate([rows_ref[b, c, x, t] for b in range(n)], axis=0).astype(f32)
            for t in range(3)
        ])

    def rs_copy(it, i, k):
        return remote(
            rs_ref.at[it, i, wrap(me + k, n)], rr_ref.at[it, i, k - 1],
            rs_send.at[i, k - 1], rs_recv.at[i, k - 1], rel(k, 0, 0),
        )

    def ag_copy(it, i, k):
        return remote(
            ag_ref.at[it, i, me], ag_ref.at[it, i, me],
            ag_send.at[i, k - 1], ag_recv.at[i, k - 1], rel(k, 0, 0),
        )

    def ag_in(it, i, k):
        at = ag_ref.at[it, i, wrap(me - k, n)]
        return remote(at, at, ag_send.at[i, k - 1], ag_recv.at[i, k - 1], rel(k, 0, 0))

    def tv_copy(i):
        return remote(g_ref.at[0, i], tv_ref.at[i], tv_send.at[i], tv_recv.at[i], rel(0, 1, 0))

    def combine(it, i):
        x = lax.rem(i, readout)
        pr = jnp.zeros((slices, lines), f32)
        pi = jnp.zeros((slices, lines), f32)
        for c in range(coils):
            cr, ci = coil_of(c, x)
            qr, qi = q_ref[i, c, 0], q_ref[i, c, 1]
            pr += cr * qr + ci * qi
            pi += cr * qi - ci * qr
        for t, part in enumerate(packed(pr, pi)):
            for b in range(n):
                cut = part[b * depth : (b + 1) * depth]
                own_ref[i, b, t] = cut
                rs_ref[it, i, b, t] = cut.astype(bf16)
        for k in range(1, n):
            rs_copy(it, i, k).start()

    def reduce(it, i, alpha):
        for k in range(1, n):
            rs_copy(it, i, k).wait_recv()
        grads = []
        for t in range(3):
            total = own_ref[i, me, t]
            for k in range(1, n):
                total = total + rr_ref[it, i, k - 1, t].astype(f32)
            grads.append(total)
        if it > 0:
            tv_copy(i).wait_recv()
            diff = [-alpha * (tv_ref[i, t] - g_ref[0, i, t]) for t in range(3)]
            main = diff[0] * diff[0] + diff[1] * diff[1]
            rest = diff[2] * diff[2]
            rest = rest + pltpu.roll(rest, HALF, 1)
            for t, modulus in enumerate((main, main, rest)):
                scale = (-2.0 * tv_weight) / jnp.sqrt(modulus + smoothing * smoothing)
                grads[t] = grads[t] + diff[t] * scale
        square = None
        for t in range(3):
            g_ref[it, i, t] = grads[t]
            ag_ref[it, i, me, t] = grads[t].astype(bf16)
            square = grads[t] * grads[t] if square is None else square + grads[t] * grads[t]
        gg_ref[...] += square
        for k in range(1, n):
            ag_copy(it, i, k).start()
        if it == 0:
            tv_copy(i).start()

    def forward(it, i):
        e, x = i // readout, lax.rem(i, readout)
        for k in range(1, n):
            ag_in(it, i, k).wait_recv()
        vr, vi = unpacked(*[
            jnp.concatenate([ag_ref[it, i, b, t] for b in range(n)], axis=0).astype(f32)
            for t in range(3)
        ])
        prods = []
        for c in range(coils):
            cr, ci = coil_of(c, x)
            prods.append((cr * vr - ci * vi).astype(bf16))
            prods.append((cr * vi + ci * vr).astype(bf16))
        prod = jnp.concatenate(prods, axis=0)
        a = jnp.dot(prod, cy_ref[...], preferred_element_type=f32)
        b = jnp.dot(prod, sy_ref[...], preferred_element_type=f32)
        mask = mask_ref[e]
        total = jnp.zeros((slices, lines), f32)
        for c in range(coils):
            lo = 2 * slices * c
            hi = lo + slices
            mid = jnp.concatenate(
                [
                    (a[lo : lo + slices] + b[hi : hi + slices]).astype(bf16),
                    (a[hi : hi + slices] - b[lo : lo + slices]).astype(bf16),
                ],
                axis=0,
            )
            out = jnp.dot(tf_ref[...], mid, preferred_element_type=f32)
            er, ei = out[:slices] * mask, out[slices:] * mask
            e_ref[i, c, 0] = er
            e_ref[i, c, 1] = ei
            total += er * er + ei * ei
        ee_ref[...] += total

    flat = (me * nphase + ph) * nenc + en

    def ar_copy(it, j):
        return remote(
            ar_ref.at[it, flat], ar_ref.at[it, flat], ar_send.at[it, j], ar_recv.at[it, j],
            rel(*offsets[j]),
        )

    def ar_in(it, j):
        a, b, c = offsets[j]
        frm = (wrap(me - a, n) * nphase + wrap(ph - b, nphase)) * nenc + wrap(en - c, nenc)
        at = ar_ref.at[it, frm]
        return remote(at, at, ar_send.at[it, j], ar_recv.at[it, j], rel(*offsets[j]))

    def step_size(it):
        gg = jnp.sum(jnp.sum(gg_ref[...], axis=0, keepdims=True), axis=1, keepdims=True)
        ee = jnp.sum(jnp.sum(ee_ref[...], axis=0, keepdims=True), axis=1, keepdims=True)
        row = lax.broadcasted_iota(jnp.int32, ar_ref.shape[2:], 0)
        ar_ref[it, flat] = jnp.where(row == 0, gg, ee)
        for j in range(len(offsets)):
            ar_copy(it, j).start()
        gg_ref[...] = jnp.zeros_like(gg_ref)
        ee_ref[...] = jnp.zeros_like(ee_ref)
        for j in range(len(offsets)):
            ar_in(it, j).wait_recv()
        total = ar_ref[it, 0]
        for s in range(1, n * nphase * nenc):
            total = total + ar_ref[it, s]
        gg, ee = total[0:1, 0:1], total[1:2, 0:1]
        alpha = gg / (ee + 4.0 * tv_weight / smoothing * gg + 1e-06)
        a_ref[it] = jnp.broadcast_to(alpha, a_ref.shape[1:])
        return alpha

    def finish_sends(it):
        @pl.loop(0, pieces)
        def _(i):
            for k in range(1, n):
                rs_copy(it, i, k).wait_send()
                ag_copy(it, i, k).wait_send()
            if it == 0:
                tv_copy(i).wait_send()

        for j in range(len(offsets)):
            ar_copy(it, j).wait_send()

    def sweep(it, alpha):
        @pl.loop(0, pieces + 2 * LAG)
        def _(s):
            @pl.when(s < pieces)
            def _():
                if it > 0:
                    transform(s, alpha)
                combine(it, s)

            @pl.when((s >= LAG) & (s < pieces + LAG))
            def _():
                reduce(it, s - LAG, alpha)

            @pl.when(s >= 2 * LAG)
            def _():
                forward(it, s - 2 * LAG)

    load_k(0).wait()

    @pl.loop(0, readout)
    def _(i):
        transform(i, None)

    pl.semaphore_wait(barrier, len(offsets))
    for k in range(1, n):
        coil_z(k).start()
    for e in range(1, encs):
        load_k(e).wait()

    @pl.loop(readout, pieces)
    def _(i):
        transform(i, None)

    for k in range(1, n):
        coil_z_in(k).wait_recv()
        coil_x(k, quarter).start()
        coil_c(k, quarter, 0).start()
    for k in range(1, n):
        coil_x(k, across).wait_recv()
        coil_c(k, across, 1).start()
    partner = wrap(en + 1, nenc)
    for k in range(1, n):
        coil_c(k, ph * nenc + partner, 0).wait_recv()
        coil_c(k, wrap(ph + 1, nphase) * nenc + partner, 1).wait_recv()

    sweep(0, None)
    alpha0 = step_size(0)
    finish_sends(0)
    sweep(1, alpha0)
    step_size(1)

    finish_sends(1)
    for k in range(1, n):
        coil_z(k).wait_send()
        coil_x(k, quarter).wait_send()
        coil_c(k, quarter, 0).wait_send()
        coil_c(k, across, 1).wait_send()


def fused_body(shape, kspace_data, coil_maps, sampling):
    n, nphase, nenc = shape["slab"], shape["phase"], shape["enc"]
    encs, row_count, slices, lines = kspace_data.shape[2:]
    readout, depth = coil_maps.shape[2:4]
    coils = row_count // readout
    pieces = encs * readout
    group = n * nphase * nenc
    cy, sy = host_table(lines)
    cz, sz = host_table(slices)
    inv = np.block([[cz, -sz], [sz, cz]])
    fwd = np.block([[cz, sz], [-sz, cz]])
    f32, bf16 = jnp.float32, jnp.bfloat16
    dma = pltpu.SemaphoreType.DMA
    vmem = pl.BlockSpec(memory_space=pltpu.VMEM)
    anywhere = pl.BlockSpec(memory_space=pl.ANY)
    left, steps, grads, alphas = pl.pallas_call(
        functools.partial(fused, (n, nphase, nenc)),
        out_shape=[
            KEEP(kspace_data.shape, f32),
            KEEP((pieces, coils, 2, slices, lines), f32),
            KEEP((ITERS, pieces, 3, depth, 2 * HALF), f32),
            KEEP((ITERS, 8, 128), f32),
        ],
        in_specs=[anywhere] * 3 + [vmem] * 4,
        out_specs=[vmem] * 4,
        scratch_shapes=[
            pltpu.VMEM(kspace_data.shape, bf16),
            pltpu.VMEM(coil_maps.shape, bf16),
            pltpu.VMEM(sampling.shape, jnp.int32),
            pltpu.VMEM((coils * n, 3, depth, 2 * HALF), bf16),
            pltpu.VMEM((n, coils, readout, 3, depth, 2 * HALF), bf16),
            pltpu.VMEM((encs, slices, lines), f32),
            pltpu.VMEM((pieces, coils, 2, slices, lines), f32),
            pltpu.VMEM((ITERS, pieces, n, 3, depth, 2 * HALF), bf16),
            pltpu.VMEM((ITERS, pieces, n - 1, 3, depth, 2 * HALF), bf16),
            pltpu.VMEM((pieces, n, 3, depth, 2 * HALF), f32),
            pltpu.VMEM((ITERS, pieces, n, 3, depth, 2 * HALF), bf16),
            pltpu.VMEM((pieces, 3, depth, 2 * HALF), f32),
            pltpu.VMEM((ITERS, group, 8, 128), f32),
            pltpu.VMEM((depth, 2 * HALF), f32),
            pltpu.VMEM((slices, lines), f32),
            dma((2 + encs,)),
            dma((n - 1,)),
            dma((n - 1,)),
            dma((n - 1,)),
            dma((n - 1,)),
            dma((2, n - 1)),
            dma((2, n - 1)),
            dma((pieces, n - 1)),
            dma((pieces, n - 1)),
            dma((pieces, n - 1)),
            dma((pieces, n - 1)),
            dma((pieces,)),
            dma((pieces,)),
            dma((ITERS, group - 1)),
            dma((ITERS, group - 1)),
        ],
        compiler_params=pltpu.CompilerParams(
            collective_id=0, has_side_effects=True, vmem_limit_bytes=LIMIT
        ),
    )(kspace_data, coil_maps, sampling, jnp.asarray(cy), jnp.asarray(sy), jnp.asarray(inv), jnp.asarray(fwd))
    return pl.pallas_call(
        finish,
        out_shape=[
            jax.ShapeDtypeStruct((2, 1, encs, readout, depth, lines), f32),
            jax.ShapeDtypeStruct(kspace_data.shape, f32),
        ],
        in_specs=[vmem] * 4,
        out_specs=[vmem, anywhere],
        scratch_shapes=[pltpu.VMEM(kspace_data.shape, f32), dma((2, encs))],
        compiler_params=pltpu.CompilerParams(vmem_limit_bytes=TAIL_LIMIT),
    )(left, steps, grads, alphas)


def chosen(shape, kspace_data, coil_maps, sampling):
    readout, depth = coil_maps.shape[2:4]
    fits = (
        shape["phase"] == 2
        and kspace_data.shape[1] == 1
        and shape["enc"] == 2
        and readout == shape["phase"] * shape["enc"]
        and kspace_data.shape[3] % readout == 0
        and depth % 16 == 0
        and coil_maps.shape[4] == 3 * HALF
        and shape["slab"] > 1
    )
    if fits:
        return fused_body(shape, kspace_data, coil_maps, sampling)
    return body(kspace_data, coil_maps, sampling)


def solution(mesh):
    in_specs = (
        P("pat", "phase", "enc", "slab", None, None),
        P("pat", None, None, "slab", None),
        P("phase", "enc", "pat", None),
    )
    out_specs = (
        P("pat", "phase", "enc", None, "slab", None),
        P("pat", "phase", "enc", "slab", None, None),
    )
    return jax.shard_map(functools.partial(chosen, dict(mesh.shape)), mesh=mesh, in_specs=in_specs, out_specs=out_specs, check_vma=False)
```

```python
import functools
import math

import jax
import jax.numpy as jnp
import numpy as np
from jax import lax
from jax.experimental import pallas as pl
from jax.experimental.pallas import tpu as pltpu
from jax.sharding import PartitionSpec as P

ITERS = 2


tv_weight = 0.15
smoothing = 0.6


def with_halo(value, sides, width):
    for axis, dim in sides:
        size, length = (lax.axis_size(axis), value.shape[dim])
        up = [(i, (i + 1) % size) for i in range(size)]
        down = [(j, i) for i, j in up]
        last = lax.slice_in_dim(value, length - width, length, axis=dim)
        first = lax.slice_in_dim(value, 0, width, axis=dim)
        before = lax.ppermute(last, axis, up)
        after = lax.ppermute(first, axis, down)
        value = jnp.concatenate([before, value, after], axis=dim)
    return value


def dft_table(length, direction):
    counter = jnp.arange(length, dtype=jnp.int32)
    product = counter[:, None] * counter[None, :] % length
    angle = product.astype(jnp.float32) * (2.0 * math.pi / length)
    factor = 1.0 / math.sqrt(length)
    return (
        (jnp.cos(angle) * factor).astype(jnp.bfloat16),
        (direction * jnp.sin(angle) * factor).astype(jnp.bfloat16),
    )


def along_rows(real_part, imag_part, table):
    cosine, sine = table
    real_out = jnp.matmul(real_part, cosine, preferred_element_type=jnp.float32) - jnp.matmul(
        imag_part, sine, preferred_element_type=jnp.float32
    )
    imag_out = jnp.matmul(real_part, sine, preferred_element_type=jnp.float32) + jnp.matmul(
        imag_part, cosine, preferred_element_type=jnp.float32
    )
    return (real_out, imag_out)


def along_depth(real_part, imag_part, table):
    cosine, sine = table
    real_out = jnp.einsum(
        "...zy,zw->...wy", real_part, cosine, preferred_element_type=jnp.float32
    ) - jnp.einsum("...zy,zw->...wy", imag_part, sine, preferred_element_type=jnp.float32)
    imag_out = jnp.einsum(
        "...zy,zw->...wy", real_part, sine, preferred_element_type=jnp.float32
    ) + jnp.einsum("...zy,zw->...wy", imag_part, cosine, preferred_element_type=jnp.float32)
    return (real_out, imag_out)


def coil_product(coil_real, coil_imag, real_in, imag_in, column_fwd):
    prod_real = (coil_real * real_in - coil_imag * imag_in).astype(jnp.bfloat16)
    prod_imag = (coil_real * imag_in + coil_imag * real_in).astype(jnp.bfloat16)
    mid_real, mid_imag = along_rows(prod_real, prod_imag, column_fwd)
    return jnp.stack([mid_real, mid_imag]).astype(jnp.bfloat16)


def body(kspace_data, coil_maps, sampling):
    phases = kspace_data.shape[1]
    encodings = kspace_data.shape[2]
    coils = coil_maps.shape[1]
    readout = coil_maps.shape[2]
    zdepth = coil_maps.shape[3]
    lines = coil_maps.shape[4]
    slices = kspace_data.shape[4]
    column_fwd = dft_table(lines, -1.0)
    depth_fwd = dft_table(slices, -1.0)
    column_inv = dft_table(lines, 1.0)
    depth_inv = dft_table(slices, 1.0)
    coil_real = coil_maps[0].astype(jnp.float32)
    coil_imag = coil_maps[1].astype(jnp.float32)
    sampled = sampling.astype(jnp.float32)[None, :, :, None]
    residual = -(kspace_data.astype(jnp.float32) * sampled)
    image_estimate = jnp.zeros((2, phases, encodings, readout, zdepth, lines), jnp.float32)
    row_count = kspace_data.shape[3]
    coil_rows = lax.all_to_all(
        coil_maps.reshape(2, coils * readout, zdepth, lines),
        "slab",
        split_axis=1,
        concat_axis=2,
        tiled=True,
    )
    row_columns = (
        lax.axis_index("slab") * row_count + jnp.arange(row_count, dtype=jnp.int32)
    ) % readout
    for iteration in range(ITERS):
        low = residual.astype(jnp.bfloat16)
        inv_real, inv_imag = along_depth(low[0], low[1], depth_inv)
        partial_rows = jnp.stack([inv_real, inv_imag]).astype(jnp.bfloat16)
        portion = lax.all_to_all(partial_rows, "slab", split_axis=4, concat_axis=3, tiled=True)
        shaped = portion.reshape(
            2,
            portion.shape[1],
            portion.shape[2],
            coils,
            readout,
            portion.shape[4],
            portion.shape[5],
        )
        fine_real, fine_imag = along_rows(shaped[0], shaped[1], column_inv)
        grad_real = jnp.sum(coil_real * fine_real + coil_imag * fine_imag, axis=2)
        grad_imag = jnp.sum(coil_real * fine_imag - coil_imag * fine_real, axis=2)
        adjoint = jnp.stack([grad_real, grad_imag])
        padded = with_halo(image_estimate, (("phase", 1),), 1)
        difference = padded[:, 1:] - padded[:, :-1]
        modulus = difference[0] * difference[0] + difference[1] * difference[1]
        weights = difference / jnp.sqrt(modulus + smoothing * smoothing)[None]
        gradient = adjoint + tv_weight * (weights[:, :-1] - weights[:, 1:])
        grad_local = jnp.sum(gradient * gradient)
        grad_sq = lax.psum(grad_local, ("slab", "phase", "enc"))
        low_grad = gradient.astype(jnp.bfloat16)
        picked = jnp.take(
            lax.all_gather(low_grad, "slab", axis=4, tiled=True), row_columns, axis=3
        ).astype(jnp.float32)
        local_coils = coil_rows.astype(jnp.float32)
        mid = coil_product(local_coils[0], local_coils[1], picked[0], picked[1], column_fwd)
        out_real, out_imag = along_depth(mid[0], mid[1], depth_fwd)
        spectrum = jnp.stack([out_real, out_imag])
        spectrum = spectrum * sampled
        spec_local = jnp.sum(spectrum * spectrum)
        spec_sq = lax.psum(spec_local, ("slab", "phase", "enc"))
        alpha = grad_sq / (spec_sq + 4.0 * tv_weight / smoothing * grad_sq + 1e-06)
        image_estimate = image_estimate - alpha * gradient
        residual = residual - alpha * spectrum
    return (image_estimate, residual)


MESH = pl.DeviceIdType.MESH
LAG, MIDDLE, LAST = 3, 5, 7
HALF = 64
KEEP = pltpu.VMEM
VMEM_BYTES = 67043328
SPARE = 7000000
TAIL_LIMIT = 40 * 1024 * 1024


def host_table(length):
    counter = np.arange(length)
    angle = (counter[:, None] * counter[None, :] % length).astype(np.float32) * np.float32(
        2.0 * math.pi / length
    )
    factor = np.float32(1.0 / math.sqrt(length))
    return (
        (np.cos(angle) * factor).astype(jnp.bfloat16),
        (np.sin(angle) * factor).astype(jnp.bfloat16),
    )


def packed(real, imag):
    full = real.shape[1] - HALF
    mixed = jnp.concatenate([real[:, full:], imag[:, full:]], axis=1)
    return [real[:, :full], imag[:, :full], mixed]


def unpacked(first, second, mixed):
    return (
        jnp.concatenate([first, mixed[:, :HALF]], axis=1),
        jnp.concatenate([second, mixed[:, HALF:]], axis=1),
    )


def finish(r_ref, e_ref, g_ref, a_ref, img_ref, res_ref, stage_ref, sems):
    readout = img_ref.shape[3]
    pieces, coils = e_ref.shape[:2]
    encs = img_ref.shape[2]
    alpha0, alpha1 = a_ref[0, 0:1, 0:1], a_ref[1, 0:1, 0:1]

    def out(ri, e):
        return pltpu.make_async_copy(stage_ref.at[ri, 0, e], res_ref.at[ri, 0, e], sems.at[ri, e])

    for ri in range(2):
        for e in range(encs):
            @pl.loop(0, readout)
            def _(x):
                for c in range(coils):
                    r = c * readout + x
                    stage_ref[ri, 0, e, r] = (
                        r_ref[ri, 0, e, r] - alpha1 * e_ref[e * readout + x, c, ri]
                    )

            out(ri, e).start()
    for i in range(pieces):
        parts = [-alpha0 * g_ref[0, i, t] - alpha1 * g_ref[1, i, t] for t in range(3)]
        real, imag = unpacked(*parts)
        img_ref[0, 0, i // readout, i % readout] = real
        img_ref[1, 0, i // readout, i % readout] = imag
    for ri in range(2):
        for e in range(encs):
            out(ri, e).wait()


def fused(sizes, k_hbm, coil_hbm, samp_hbm, cy_hbm, sy_hbm, ti_hbm, tf_hbm, res_ref, e_ref, g_ref,
          a_ref, k_ref, coil_ref, samp_ref, pack_ref,
          rows_ref, mask_ref, q_ref, rs_ref, rr_ref, own_ref, ag_ref, tv_ref,
          ar_ref, gg_ref, ee_ref, cy_ref, sy_ref, ti_ref, tf_ref,
          in_sem, cz_send, cz_recv, cx_send, cx_recv, cc_send, cc_recv,
          rs_send, rs_recv, ag_send, ag_recv, tv_send, tv_recv, ar_send, ar_recv):
    n, nphase, nenc = sizes
    readout, depth = coil_ref.shape[2], coil_ref.shape[3]
    encs = k_ref.shape[2]
    slices, lines = k_ref.shape[4], k_ref.shape[5]
    coils = k_ref.shape[3] // readout
    pieces = encs * readout
    me = lax.axis_index("slab")
    ph = lax.axis_index("phase")
    en = lax.axis_index("enc")
    f32, bf16 = jnp.float32, jnp.bfloat16

    def wrap(value, size):
        return lax.rem(value + size, size)

    offsets = [
        (a, b, c)
        for a in range(n)
        for b in range(nphase)
        for c in range(nenc)
        if (a, b, c) != (0, 0, 0)
    ]

    def rel(a, b, c):
        return {"slab": wrap(me + a, n), "phase": wrap(ph + b, nphase), "enc": wrap(en + c, nenc)}

    def remote(src, dst, send, recv, where):
        return pltpu.make_async_remote_copy(
            src_ref=src, dst_ref=dst, send_sem=send, recv_sem=recv, device_id=where,
            device_id_type=MESH,
        )

    barrier = pltpu.get_barrier_semaphore()
    for off in offsets:
        pl.semaphore_signal(barrier, inc=1, device_id=rel(*off), device_id_type=MESH)

    quarter = ph * nenc + en
    across = wrap(ph + 1, nphase) * nenc + en

    def coil_z(k):
        to = wrap(me + k, n)
        return remote(
            pack_ref.at[pl.ds(to * coils, coils)], rows_ref.at[me, :, quarter],
            cz_send.at[k - 1], cz_recv.at[k - 1], rel(k, 0, 0),
        )

    def coil_z_in(k):
        frm = wrap(me - k, n)
        return remote(
            pack_ref.at[pl.ds(0, coils)], rows_ref.at[frm, :, quarter],
            cz_send.at[k - 1], cz_recv.at[k - 1], rel(k, 0, 0),
        )

    def coil_x(k, which):
        at = rows_ref.at[wrap(me - k, n), :, which]
        return remote(at, at, cx_send.at[k - 1], cx_recv.at[k - 1], rel(0, 1, 0))

    def coil_c(k, which, s):
        at = rows_ref.at[wrap(me - k, n), :, which]
        return remote(at, at, cc_send.at[s, k - 1], cc_recv.at[s, k - 1], rel(0, 0, 1))

    def load_k(e):
        return pltpu.make_async_copy(k_hbm.at[:, :, e], k_ref.at[:, :, e], in_sem.at[2 + e])

    load_coil = pltpu.make_async_copy(coil_hbm, coil_ref, in_sem.at[0])
    load_samp = pltpu.make_async_copy(samp_hbm, samp_ref, in_sem.at[1])
    tables = [
        pltpu.make_async_copy(src, dst, in_sem.at[2 + encs + t])
        for t, (src, dst) in enumerate(
            ((cy_hbm, cy_ref), (sy_hbm, sy_ref), (ti_hbm, ti_ref), (tf_hbm, tf_ref))
        )
    ]
    load_coil.start()
    load_samp.start()
    for table in tables:
        table.start()
    for e in range(encs):
        load_k(e).start()
    load_coil.wait()

    @pl.loop(0, coils * n)
    def _(c):
        for t, part in enumerate(packed(coil_ref[0, c, quarter].astype(f32), coil_ref[1, c, quarter].astype(f32))):
            pack_ref[c, t] = part.astype(bf16)

    @pl.loop(0, coils)
    def _(c):
        source = me * coils + c
        for x in range(readout):
            parts = packed(coil_ref[0, source, x].astype(f32), coil_ref[1, source, x].astype(f32))
            for t, part in enumerate(parts):
                rows_ref[me, c, x, t] = part.astype(bf16)

    load_samp.wait()
    for table in tables:
        table.wait()
    mask_ref[...] = samp_ref[0].astype(f32)
    gg_ref[...] = jnp.zeros_like(gg_ref)
    ee_ref[...] = jnp.zeros_like(ee_ref)

    def transform(i, alpha):
        e, x = i // readout, lax.rem(i, readout)
        mask = mask_ref[e]
        mids = []
        for c in range(coils):
            r = c * readout + x
            parts = []
            for ri in range(2):
                value = -(k_ref[ri, 0, e, r].astype(f32) * mask)
                if alpha is not None:
                    value = value - alpha * e_ref[i, c, ri]
                    res_ref[ri, 0, e, r] = value
                parts.append(value.astype(bf16))
            stacked = jnp.concatenate(parts, axis=0)
            mids.append(
                jnp.dot(ti_ref[...], stacked, preferred_element_type=f32).astype(bf16)
            )
        mid = jnp.concatenate(mids, axis=0)
        a = jnp.dot(mid, cy_ref[...], preferred_element_type=f32)
        b = jnp.dot(mid, sy_ref[...], preferred_element_type=f32)
        for c in range(coils):
            lo = 2 * slices * c
            hi = lo + slices
            q_ref[i, c, 0] = a[lo : lo + slices] - b[hi : hi + slices]
            q_ref[i, c, 1] = b[lo : lo + slices] + a[hi : hi + slices]

    def coil_of(c, x):
        return unpacked(*[
            jnp.concatenate([rows_ref[b, c, x, t] for b in range(n)], axis=0).astype(f32)
            for t in range(3)
        ])

    def rs_copy(it, i, k):
        return remote(
            rs_ref.at[it, i, wrap(me + k, n)], rr_ref.at[it, i, k - 1],
            rs_send.at[i, k - 1], rs_recv.at[i, k - 1], rel(k, 0, 0),
        )

    beside = me + 1 - 2 * lax.rem(me, 2)
    opposite = wrap(me + 2, n)
    near, over = wrap(beside - me, n), 2

    def ag_send_to(it, i, block, which):
        at = ag_ref.at[it, i, block]
        return remote(
            at, at, ag_send.at[i, which], ag_recv.at[i, which],
            rel(over if which == 1 else near, 0, 0),
        )

    def ag_near(it, i):
        return ag_send_to(it, i, me, 0)

    def ag_near_in(it, i):
        return ag_send_to(it, i, beside, 0)

    def ag_over(it, i):
        return ag_send_to(it, i, me, 1)

    def ag_over_in(it, i):
        return ag_send_to(it, i, opposite, 1)

    def ag_relay(it, i):
        return ag_send_to(it, i, opposite, 2)

    def ag_relay_in(it, i):
        return ag_send_to(it, i, wrap(beside + 2, n), 2)

    def tv_copy(i):
        return remote(g_ref.at[0, i], tv_ref.at[i], tv_send.at[i], tv_recv.at[i], rel(0, 1, 0))

    def combine(it, i):
        x = lax.rem(i, readout)
        pr = jnp.zeros((slices, lines), f32)
        pi = jnp.zeros((slices, lines), f32)
        for c in range(coils):
            cr, ci = coil_of(c, x)
            qr, qi = q_ref[i, c, 0], q_ref[i, c, 1]
            pr += cr * qr + ci * qi
            pi += cr * qi - ci * qr
        for t, part in enumerate(packed(pr, pi)):
            for b in range(n):
                cut = part[b * depth : (b + 1) * depth]
                own_ref[i, b, t] = cut
                rs_ref[it, i, b, t] = cut.astype(bf16)
        for k in range(1, n):
            rs_copy(it, i, k).start()

    def reduce(it, i, alpha):
        for k in range(1, n):
            rs_copy(it, i, k).wait_recv()
        grads = []
        for t in range(3):
            total = own_ref[i, me, t]
            for k in range(1, n):
                total = total + rr_ref[it, i, k - 1, t].astype(f32)
            grads.append(total)
        if it > 0:
            tv_copy(i).wait_recv()
            diff = [-alpha * (tv_ref[i, t] - g_ref[0, i, t]) for t in range(3)]
            main = diff[0] * diff[0] + diff[1] * diff[1]
            rest = diff[2] * diff[2]
            rest = rest + pltpu.roll(rest, HALF, 1)
            for t, modulus in enumerate((main, main, rest)):
                scale = (-2.0 * tv_weight) / jnp.sqrt(modulus + smoothing * smoothing)
                grads[t] = grads[t] + diff[t] * scale
        square = None
        for t in range(3):
            g_ref[it, i, t] = grads[t]
            ag_ref[it, i, me, t] = grads[t].astype(bf16)
            square = grads[t] * grads[t] if square is None else square + grads[t] * grads[t]
        gg_ref[...] += square
        ag_over(it, i).start()
        ag_near(it, i).start()
        if it == 0:
            tv_copy(i).start()

    def forward(it, i):
        e, x = i // readout, lax.rem(i, readout)
        ag_near_in(it, i).wait_recv()
        ag_relay_in(it, i).wait_recv()
        vr, vi = unpacked(*[
            jnp.concatenate([ag_ref[it, i, b, t] for b in range(n)], axis=0).astype(f32)
            for t in range(3)
        ])
        prods = []
        for c in range(coils):
            cr, ci = coil_of(c, x)
            prods.append((cr * vr - ci * vi).astype(bf16))
            prods.append((cr * vi + ci * vr).astype(bf16))
        prod = jnp.concatenate(prods, axis=0)
        a = jnp.dot(prod, cy_ref[...], preferred_element_type=f32)
        b = jnp.dot(prod, sy_ref[...], preferred_element_type=f32)
        mask = mask_ref[e]
        total = jnp.zeros((slices, lines), f32)
        for c in range(coils):
            lo = 2 * slices * c
            hi = lo + slices
            mid = jnp.concatenate(
                [
                    (a[lo : lo + slices] + b[hi : hi + slices]).astype(bf16),
                    (a[hi : hi + slices] - b[lo : lo + slices]).astype(bf16),
                ],
                axis=0,
            )
            out = jnp.dot(tf_ref[...], mid, preferred_element_type=f32)
            er, ei = out[:slices] * mask, out[slices:] * mask
            e_ref[i, c, 0] = er
            e_ref[i, c, 1] = ei
            total += er * er + ei * ei
        ee_ref[...] += total

    flat = (me * nphase + ph) * nenc + en

    def ar_copy(it, j):
        return remote(
            ar_ref.at[it, flat], ar_ref.at[it, flat], ar_send.at[it, j], ar_recv.at[it, j],
            rel(*offsets[j]),
        )

    def ar_in(it, j):
        a, b, c = offsets[j]
        frm = (wrap(me - a, n) * nphase + wrap(ph - b, nphase)) * nenc + wrap(en - c, nenc)
        at = ar_ref.at[it, frm]
        return remote(at, at, ar_send.at[it, j], ar_recv.at[it, j], rel(*offsets[j]))

    def step_size(it):
        gg = jnp.sum(jnp.sum(gg_ref[...], axis=0, keepdims=True), axis=1, keepdims=True)
        ee = jnp.sum(jnp.sum(ee_ref[...], axis=0, keepdims=True), axis=1, keepdims=True)
        row = lax.broadcasted_iota(jnp.int32, ar_ref.shape[2:], 0)
        ar_ref[it, flat] = jnp.where(row == 0, gg, ee)
        for j in range(len(offsets)):
            ar_copy(it, j).start()
        gg_ref[...] = jnp.zeros_like(gg_ref)
        ee_ref[...] = jnp.zeros_like(ee_ref)
        for j in range(len(offsets)):
            ar_in(it, j).wait_recv()
        total = ar_ref[it, 0]
        for s in range(1, n * nphase * nenc):
            total = total + ar_ref[it, s]
        gg, ee = total[0:1, 0:1], total[1:2, 0:1]
        alpha = gg / (ee + 4.0 * tv_weight / smoothing * gg + 1e-06)
        a_ref[it] = jnp.broadcast_to(alpha, a_ref.shape[1:])
        return alpha

    def finish_sends(it):
        @pl.loop(0, pieces)
        def _(i):
            for k in range(1, n):
                rs_copy(it, i, k).wait_send()
            ag_over(it, i).wait_send()
            ag_near(it, i).wait_send()
            ag_relay(it, i).wait_send()
            if it == 0:
                tv_copy(i).wait_send()

        for j in range(len(offsets)):
            ar_copy(it, j).wait_send()

    partner = wrap(en + 1, nenc)
    beyond = wrap(ph + 1, nphase)

    def piece(s):
        e, j = lax.rem(s, encs), s // encs
        x = wrap(ph + j // nenc, nphase) * nenc + wrap(en + lax.rem(j, nenc), nenc)
        return e * readout + x

    def coils_ready(s):
        @pl.when(s == encs)
        def _():
            for k in range(1, n):
                coil_c(k, ph * nenc + partner, 0).wait_recv()

        @pl.when(s == nenc * encs)
        def _():
            for k in range(1, n):
                coil_x(k, across).wait_recv()
                coil_c(k, across, 1).start()

        @pl.when(s == (nenc + 1) * encs)
        def _():
            for k in range(1, n):
                coil_c(k, beyond * nenc + partner, 1).wait_recv()

    def sweep(it, alpha):
        @pl.loop(0, pieces + LAST)
        def _(s):
            @pl.when(s < pieces)
            def _():
                p = piece(s)
                if it > 0:
                    transform(p, alpha)
                else:
                    coils_ready(s)
                combine(it, p)

            @pl.when((s >= LAG) & (s < pieces + LAG))
            def _():
                reduce(it, piece(s - LAG), alpha)

            @pl.when((s >= MIDDLE) & (s < pieces + MIDDLE))
            def _():
                p = piece(s - MIDDLE)
                ag_over_in(it, p).wait_recv()
                ag_relay(it, p).start()

            @pl.when(s >= LAST)
            def _():
                forward(it, piece(s - LAST))

    load_k(0).wait()

    @pl.loop(0, readout)
    def _(i):
        transform(i, None)

    pl.semaphore_wait(barrier, len(offsets))
    for k in range(1, n):
        coil_z(k).start()
    for e in range(1, encs):
        load_k(e).wait()

    @pl.loop(readout, pieces)
    def _(i):
        transform(i, None)

    nearest = [sorted(range(1, n), key=lambda k: abs((m - k) % n - m)) for m in range(n)]
    for j in range(n - 1):
        k = nearest[0][j]
        for m in range(1, n):
            k = jnp.where(me == m, nearest[m][j], k)
        coil_z_in(k).wait_recv()
        coil_x(k, quarter).start()
        coil_c(k, quarter, 0).start()

    sweep(0, None)
    alpha0 = step_size(0)
    finish_sends(0)
    sweep(1, alpha0)
    step_size(1)

    finish_sends(1)
    for k in range(1, n):
        coil_z(k).wait_send()
        coil_x(k, quarter).wait_send()
        coil_c(k, quarter, 0).wait_send()
        coil_c(k, across, 1).wait_send()


def fused_body(shape, kspace_data, coil_maps, sampling):
    n, nphase, nenc = shape["slab"], shape["phase"], shape["enc"]
    encs, row_count, slices, lines = kspace_data.shape[2:]
    readout, depth = coil_maps.shape[2:4]
    coils = row_count // readout
    pieces = encs * readout
    group = n * nphase * nenc
    cy, sy = host_table(lines)
    cz, sz = host_table(slices)
    inv = np.block([[cz, -sz], [sz, cz]])
    fwd = np.block([[cz, sz], [-sz, cz]])
    f32, bf16 = jnp.float32, jnp.bfloat16
    dma = pltpu.SemaphoreType.DMA
    vmem = pl.BlockSpec(memory_space=pltpu.VMEM)
    anywhere = pl.BlockSpec(memory_space=pl.ANY)
    stay = pl.BlockSpec(memory_space=pltpu.HBM)
    wide = -(-lines // 128) * 128
    kept = 4 * (2 * encs * row_count * slices * wide * 2 + ITERS * (pieces * 3 * depth * 128 + 1024))
    left, steps, grads, alphas = pl.pallas_call(
        functools.partial(fused, (n, nphase, nenc)),
        out_shape=[
            KEEP(kspace_data.shape, f32),
            KEEP((pieces, coils, 2, slices, lines), f32),
            KEEP((ITERS, pieces, 3, depth, 2 * HALF), f32),
            KEEP((ITERS, 8, 128), f32),
        ],
        in_specs=[stay] * 7,
        out_specs=[vmem] * 4,
        scratch_shapes=[
            pltpu.VMEM(kspace_data.shape, bf16),
            pltpu.VMEM(coil_maps.shape, bf16),
            pltpu.VMEM(sampling.shape, jnp.int32),
            pltpu.VMEM((coils * n, 3, depth, 2 * HALF), bf16),
            pltpu.VMEM((n, coils, readout, 3, depth, 2 * HALF), bf16),
            pltpu.VMEM((encs, slices, lines), f32),
            pltpu.VMEM((pieces, coils, 2, slices, lines), f32),
            pltpu.VMEM((ITERS, pieces, n, 3, depth, 2 * HALF), bf16),
            pltpu.VMEM((ITERS, pieces, n - 1, 3, depth, 2 * HALF), bf16),
            pltpu.VMEM((pieces, n, 3, depth, 2 * HALF), f32),
            pltpu.VMEM((ITERS, pieces, n, 3, depth, 2 * HALF), bf16),
            pltpu.VMEM((pieces, 3, depth, 2 * HALF), f32),
            pltpu.VMEM((ITERS, group, 8, 128), f32),
            pltpu.VMEM((depth, 2 * HALF), f32),
            pltpu.VMEM((slices, lines), f32),
            pltpu.VMEM((lines, lines), bf16),
            pltpu.VMEM((lines, lines), bf16),
            pltpu.VMEM((2 * slices, 2 * slices), bf16),
            pltpu.VMEM((2 * slices, 2 * slices), bf16),
            dma((6 + encs,)),
            dma((n - 1,)),
            dma((n - 1,)),
            dma((n - 1,)),
            dma((n - 1,)),
            dma((2, n - 1)),
            dma((2, n - 1)),
            dma((pieces, n - 1)),
            dma((pieces, n - 1)),
            dma((pieces, n - 1)),
            dma((pieces, n - 1)),
            dma((pieces,)),
            dma((pieces,)),
            dma((ITERS, group - 1)),
            dma((ITERS, group - 1)),
        ],
        compiler_params=pltpu.CompilerParams(
            collective_id=0, has_side_effects=True, vmem_limit_bytes=(VMEM_BYTES - kept - SPARE) // 1024 * 1024
        ),
    )(kspace_data, coil_maps, sampling, jnp.asarray(cy), jnp.asarray(sy), jnp.asarray(inv), jnp.asarray(fwd))
    return pl.pallas_call(
        finish,
        out_shape=[
            jax.ShapeDtypeStruct((2, 1, encs, readout, depth, lines), f32),
            jax.ShapeDtypeStruct(kspace_data.shape, f32),
        ],
        in_specs=[vmem] * 4,
        out_specs=[vmem, anywhere],
        scratch_shapes=[pltpu.VMEM(kspace_data.shape, f32), dma((2, encs))],
        compiler_params=pltpu.CompilerParams(vmem_limit_bytes=TAIL_LIMIT),
    )(left, steps, grads, alphas)


def chosen(shape, kspace_data, coil_maps, sampling):
    readout, depth = coil_maps.shape[2:4]
    fits = (
        shape["phase"] == 2
        and kspace_data.shape[1] == 1
        and shape["enc"] == 2
        and readout == shape["phase"] * shape["enc"]
        and kspace_data.shape[3] % readout == 0
        and depth % 16 == 0
        and coil_maps.shape[4] == 3 * HALF
        and shape["slab"] == 4
    )
    if fits:
        return fused_body(shape, kspace_data, coil_maps, sampling)
    return body(kspace_data, coil_maps, sampling)


def solution(mesh):
    in_specs = (
        P("pat", "phase", "enc", "slab", None, None),
        P("pat", None, None, "slab", None),
        P("phase", "enc", "pat", None),
    )
    out_specs = (
        P("pat", "phase", "enc", None, "slab", None),
        P("pat", "phase", "enc", "slab", None, None),
    )
    return jax.shard_map(functools.partial(chosen, dict(mesh.shape)), mesh=mesh, in_specs=in_specs, out_specs=out_specs, check_vma=False)
```
